32 devices in a mesh: grp: 8 (over z, x), sub: 4 (over y, core).
Axes of the slice: x: 2, y: 2, z: 4, core: 2. Of those that a mesh axis runs over, the one named last changes fastest.
Arguments:
- child_moments: bfloat16 [294, 32768], P(None, ('grp', 'sub')), may hold values from -6 to 6
- upward_matrix: bfloat16 [294, 8, 294], replicated, may hold values from -0.125 to 0.125
- project_matrix: bfloat16 [64, 294], replicated, may hold values from -0.375 to 0.375
- transfer_matrix: bfloat16 [64, 20224], replicated, may hold values from -0.0546875 to 0.0546875
- expand_matrix: bfloat16 [294, 64], replicated, may hold values from -0.75 to 0.75
- downward_matrix: bfloat16 [294, 8, 294], replicated, may hold values from -0.375 to 0.375
- neighbour_list: int32 [316, 4096], P(None, ('grp', 'sub')), may hold values from 0 to 832, as said below
- ghost_map: int32 [32, 80], P(('grp', 'sub')), may hold values from 0 to 128, as said below
Outputs:
- child_locals: bfloat16 [294, 32768], P(None, ('grp', 'sub'))
The draws below stay inside these ranges and needn't reach their ends.
Inputs may be any that keep to these rules, and one draw needn't show every extreme that they name: `neighbour_list`: entries below 832 name a source slot; each column has between 95 and 189 such entries, and the first column of every device's block has exactly 189. Every ghost slot that is named holds a box. `ghost_map`: the groups stand in a three-dimensional arrangement; a device sends boxes only to groups next to its own there (all other destinations hold 128 only). Slot 0 of every such destination names a box, and every device fills all 10 slots of at least one destination.
All inputs are finite; a program needn't handle non-finite values.
Results may differ from the reference program's by a relative error of at most 0.0085.
Values may be sent and summed in bfloat16 or wider, within the bound.
No kernel may reach another device: no remote copies, remote signals or barrier semaphores. Data moves between devices by JAX's collectives and lax.ppermute only.
A program may use at most 64 MiB of HBM per device.

```python
import jax
import jax.numpy as jnp
from jax import lax

NE = 98
RANK = 64
OFFS = 316
VLIST = 189
GHOST = 10
BOX_DEV = 128
SENDERS = 32
TARGETS = 4096
CHILDREN = 32768
GROUP_SLOTS = 80
POOL = 832
N_GRP = 8
N_SUB = 4


def group_shape():
    half = N_GRP // 2
    rows = 1
    for cand in range(1, half + 1):
        if half % cand == 0 and cand * cand <= half:
            rows = cand
    return (half, half // rows)


def ghost_table(key):
    half, cols = group_shape()
    groups = jnp.arange(N_GRP, dtype=jnp.int32)
    layer = groups // half
    row_pos = groups % half // cols
    col_pos = groups % cols
    near = (jnp.abs(layer[:, None] - layer[None, :]) <= 1) & (jnp.abs(row_pos[:, None] - row_pos[None, :]) <= 1)
    near = near & (jnp.abs(col_pos[:, None] - col_pos[None, :]) <= 1) & (groups[:, None] != groups[None, :])
    sender_group = jnp.arange(SENDERS, dtype=jnp.int32) // N_SUB
    near_send = near[sender_group]
    partner = (sender_group + half) % N_GRP
    count = jax.random.randint(jax.random.fold_in(key, 31), (SENDERS, N_GRP), 1, GHOST + 1)
    count = jnp.where(groups[None, :] == partner[:, None], GHOST, count)
    box_ids = jax.random.randint(jax.random.fold_in(key, 32), (SENDERS, N_GRP, GHOST), 0, BOX_DEV)
    slot_index = jnp.arange(GHOST, dtype=jnp.int32).reshape(1, 1, GHOST)
    live = near_send[:, :, None] & (slot_index < count[:, :, None])
    return jnp.where(live, box_ids, BOX_DEV).astype(jnp.int32)


def draw_ghost_map(key, part):
    return ghost_table(key).reshape(SENDERS, GROUP_SLOTS).astype(jnp.int32)


def draw_neighbour_list(key, part):
    group_boxes = N_SUB * BOX_DEV
    ghost_total = N_SUB * N_GRP * GHOST
    table = ghost_table(key).reshape(N_GRP, N_SUB, N_GRP, GHOST)
    live = jnp.transpose(table, (2, 1, 0, 3)).reshape(N_GRP, ghost_total) < BOX_DEV
    ranks = jnp.where(live, 0, 1) * ghost_total + jnp.arange(ghost_total, dtype=jnp.int32)[None, :]
    order = jnp.argsort(ranks, axis=1).astype(jnp.int32)
    live_total = jnp.sum(live.astype(jnp.int32), axis=1)
    target_group = jnp.arange(TARGETS, dtype=jnp.int32) // group_boxes
    bits = jax.random.randint(jax.random.fold_in(key, 24), (OFFS, TARGETS), 0, 1 << 20)
    pick = bits % live_total[target_group][None, :]
    ghost_col = order[target_group[None, :], pick] + group_boxes
    own_col = jax.random.randint(jax.random.fold_in(key, 25), (OFFS, TARGETS), 0, group_boxes)
    use_own = jax.random.randint(jax.random.fold_in(key, 26), (OFFS, TARGETS), 0, 2) == 1
    source = jnp.where(use_own, own_col, ghost_col)
    live_count = VLIST - jax.random.randint(jax.random.fold_in(key, 21), (TARGETS,), 0, VLIST // 2 + 1)
    first_box = jnp.arange(TARGETS) % BOX_DEV == 0
    live_count = jnp.where(first_box, VLIST, live_count)
    scores = jax.random.randint(jax.random.fold_in(key, 22), (OFFS, TARGETS), 0, 1 << 20) * OFFS + jnp.arange(OFFS).reshape(OFFS, 1)
    ranking = jnp.argsort(scores, axis=0)
    position = jnp.argsort(ranking, axis=0)
    return jnp.where(position < live_count[None, :], source, POOL).astype(jnp.int32)


def steps_of(key, extent, shards, low, high):
    gain, own = 1.0, jax.random.fold_in(key, 6)
    for axis_at, blocks in shards:
        steps = jnp.exp(jax.random.uniform(jax.random.fold_in(own, axis_at), (blocks,), jnp.float32, low / len(shards), high / len(shards)))
        gain = gain * jnp.repeat(steps, extent[axis_at] // blocks).reshape([-1 if axis == axis_at else 1 for axis in range(len(extent))])
    return gain


def noise(rng, shape, scale, most, pieces=(), held_as=jnp.bfloat16):
    values = scale * jax.random.normal(rng, shape, jnp.float32)
    if pieces:
        values = values * steps_of(rng, shape, pieces, -0.22, 0.18)
    return jnp.clip(values, -most, most).astype(held_as)


def setup_inputs(seed: int = 0) -> dict:
    splits = jax.random.split(jax.random.key(seed), 9)
    child_moments = noise(splits[0], (3 * NE, CHILDREN), 1.0, 6.0, ((1, 32),))
    upward_matrix = noise(splits[1], (3 * NE, 8, 3 * NE), (24 * NE) ** -0.5, 0.125)
    project_matrix = noise(splits[2], (RANK, 3 * NE), (3 * NE) ** -0.5, 0.375)
    transfer_matrix = noise(splits[3], (RANK, OFFS * RANK), (VLIST * RANK) ** -0.5, 0.0546875)
    expand_matrix = noise(splits[4], (3 * NE, RANK), RANK ** -0.5, 0.75)
    downward_matrix = noise(splits[5], (3 * NE, 8, 3 * NE), (3 * NE) ** -0.5, 0.375)
    neighbour_list = draw_neighbour_list(jax.random.fold_in(splits[8], 71), 0)
    ghost_map = draw_ghost_map(jax.random.fold_in(splits[8], 71), 0)
    return {"child_moments": child_moments, "upward_matrix": upward_matrix, "project_matrix": project_matrix, "transfer_matrix": transfer_matrix, "expand_matrix": expand_matrix, "downward_matrix": downward_matrix, "neighbour_list": neighbour_list, "ghost_map": ghost_map}


def reference(child_moments, upward_matrix, project_matrix, transfer_matrix, expand_matrix, downward_matrix, neighbour_list, ghost_map):
    surface = 3 * NE
    group_boxes = N_SUB * BOX_DEV
    upward_float = upward_matrix.astype(jnp.float32)
    downward_float = downward_matrix.astype(jnp.float32)
    children = jnp.moveaxis(child_moments.reshape(surface, N_GRP, N_SUB, 8, BOX_DEV), 1, 0)

    def upward(group_block):
        parent = jnp.einsum("icj,jscb->isb", upward_float, group_block.astype(jnp.float32)).astype(jnp.bfloat16)
        return jnp.dot(project_matrix, parent.reshape(surface, group_boxes), preferred_element_type=jnp.float32).astype(jnp.bfloat16)

    packed = lax.map(upward, children)
    flat_packed = jnp.moveaxis(packed, 0, 1).reshape(RANK, TARGETS)
    padded = jnp.concatenate([flat_packed, jnp.zeros((RANK, 1), jnp.bfloat16)], axis=1)
    send_table = ghost_map.reshape(N_GRP, N_SUB, N_GRP, GHOST)
    device_base = (jnp.arange(N_GRP * N_SUB, dtype=jnp.int32) * BOX_DEV).reshape(N_GRP, N_SUB, 1, 1)
    ghost_column = jnp.where(send_table < BOX_DEV, device_base + send_table, TARGETS).astype(jnp.int32)
    ghost_column = jnp.transpose(ghost_column, (2, 1, 0, 3)).reshape(N_GRP, N_SUB * N_GRP * GHOST)
    neighbours = jnp.moveaxis(neighbour_list.reshape(OFFS, N_GRP, group_boxes), 1, 0)
    translate = transfer_matrix.astype(jnp.float32).reshape(RANK, OFFS, RANK)

    def downward(inputs):
        own_packed, columns, lists = inputs
        source_pool = jnp.concatenate([own_packed, padded[:, columns], jnp.zeros((RANK, 1), jnp.bfloat16)], axis=1)
        picked = source_pool[:, lists].astype(jnp.float32)
        local_coeff = jnp.einsum("roq,qot->rt", translate, picked).astype(jnp.bfloat16)
        local_moment = jnp.dot(expand_matrix, local_coeff, preferred_element_type=jnp.float32).astype(jnp.bfloat16)
        moment_float = local_moment.astype(jnp.float32).reshape(surface, N_SUB, BOX_DEV)
        return jnp.einsum("icj,jsb->iscb", downward_float, moment_float).astype(jnp.bfloat16)

    result = lax.map(downward, (packed, ghost_column, neighbours))
    return jnp.moveaxis(result, 0, 1).reshape(surface, CHILDREN)
```

```python
import functools

import jax
import jax.numpy as jnp
from jax import lax
from jax.experimental import pallas as pl
from jax.experimental.pallas import tpu as pltpu
from jax.sharding import PartitionSpec as P

LANES = 128
VMEM = pl.BlockSpec(memory_space=pltpu.VMEM)
SMEM = pl.BlockSpec(memory_space=pltpu.SMEM)


def lane_gather(values, lanes):
    numbers = lax.GatherDimensionNumbers(
        offset_dims=(),
        collapsed_slice_dims=(1,),
        start_index_map=(1,),
        operand_batching_dims=(0,),
        start_indices_batching_dims=(0,),
    )
    return lax.gather(
        values,
        lanes[..., None],
        numbers,
        slice_sizes=(1, 1),
        mode=lax.GatherScatterMode.PROMISE_IN_BOUNDS,
    )


def chunks_of(total, size):
    return [(at, min(size, total - at)) for at in range(0, total, size)]


def upward_kernel(rows_per, x_ref, u_ref, p_ref, map_ref, packed_ref, ghost_ref, wide, parent, slots):
    surface = x_ref.shape[0]
    coeff = p_ref.shape[0]
    for at, size in chunks_of(surface, 96):
        for n, (left, width) in enumerate(chunks_of(surface, LANES)):
            wide[n, pl.ds(at * 8, size * 8), 0:width] = u_ref[
                pl.ds(at * 8, size * 8), left : left + width
            ].astype(jnp.float32)
        total = jnp.zeros((size, LANES), jnp.float32)
        for c in range(8):
            matrix = jnp.concatenate(
                [
                    wide.at[n][pl.ds(at * 8 + c, size, stride=8), :].astype(jnp.bfloat16)[:, :width]
                    for n, (_, width) in enumerate(chunks_of(surface, LANES))
                ],
                axis=1,
            )
            total += jnp.dot(
                matrix,
                x_ref[:, c * LANES : (c + 1) * LANES],
                preferred_element_type=jnp.float32,
            )
        parent[pl.ds(at, size), :] = total.astype(jnp.bfloat16)
    packed = jnp.dot(p_ref[...], parent[...], preferred_element_type=jnp.float32)
    packed = packed.astype(jnp.bfloat16)
    packed_ref[...] = packed
    width = slots.shape[1]
    slots[...] = jnp.full(slots.shape, LANES, jnp.int32)
    slots[:, 0 : map_ref.shape[1]] = map_ref[...]
    for at in range(0, width, LANES):
        ids = jnp.broadcast_to(slots[:, at : at + LANES], (coeff, LANES))
        taken = lane_gather(packed, (ids & (LANES - 1)).astype(jnp.int16)).astype(jnp.float32)
        taken = jnp.where(ids < LANES, taken, 0.0)
        rows = jnp.transpose(taken).astype(jnp.bfloat16)
        keep = min(LANES, map_ref.shape[1] - at)
        ghost_ref[at : at + keep, :] = rows[:keep, :]


def pick(index_row, tile_row, tiles, pool_ref, coeff, names):
    lanes = jnp.broadcast_to(index_row, (coeff, LANES)).astype(jnp.int16)
    place = jnp.broadcast_to(tile_row, (coeff, LANES)).astype(jnp.int16)
    out = jnp.zeros((coeff, LANES), jnp.bfloat16)
    if tiles <= 8:
        for k in range(tiles):
            got = lane_gather(pool_ref[:, k * LANES : (k + 1) * LANES], lanes)
            out = jnp.where(place == names(k), got, out)
        return out

    def one(k, out):
        got = lane_gather(pool_ref[:, pl.ds(pl.multiple_of(k * LANES, LANES), LANES)], lanes)
        return jnp.where(place == names(k), got, out)

    return lax.fori_loop(0, tiles, one, out)


def translate(index, tile, matrix_ref, pool_ref, tiles, names, unroll):
    coeff = pool_ref.shape[0]
    offsets = index.shape[0]
    group = 4

    def block(at, count):
        parts = [
            pick(index[pl.ds(at + n, 1), :], tile[pl.ds(at + n, 1), :], tiles, pool_ref, coeff, names)
            for n in range(count)
        ]
        return jnp.dot(
            matrix_ref[:, pl.ds(pl.multiple_of(at * coeff, LANES) if not isinstance(at, int) else at * coeff, count * coeff)],
            jnp.concatenate(parts, axis=0),
            preferred_element_type=jnp.float32,
        )

    step = group * unroll
    trips = offsets // step

    def body(i, total):
        for n in range(unroll):
            total += block(i * step + n * group, group)
        return total

    total = lax.fori_loop(0, trips, body, jnp.zeros((coeff, LANES), jnp.float32))
    for at, count in chunks_of(offsets - trips * step, group):
        total += block(trips * step + at, count)
    return total


def own_kernel(me_ref, list_ref, matrix_ref, pool_ref, out_ref, index, tile):
    me = me_ref[0, 0]
    lists = list_ref[...]
    index[...] = lists & (LANES - 1)
    tile[...] = (lists // LANES) ^ me
    tiles = pool_ref.shape[1] // LANES
    out_ref[...] = translate(
        index, tile, matrix_ref, pool_ref, tiles, lambda k: jnp.int16(k), 4
    )


def ghost_kernel(
    own_boxes, list_ref, matrix_ref, rows_ref, own_ref, e_ref, d_ref, out_ref, index, tile, pool, wide
):
    coeff = matrix_ref.shape[0]
    surface = e_ref.shape[0]
    count = rows_ref.shape[0]
    lists = list_ref[...] - own_boxes
    index[...] = lists & (LANES - 1)
    tile[...] = jnp.where((lists >= 0) & (lists < count), lists >> 7, -1)
    for at, size in chunks_of(count, LANES):
        rows = rows_ref[at : at + size, :].astype(jnp.float32)
        if size < LANES:
            rows = jnp.concatenate([rows, jnp.zeros((LANES - size, coeff), jnp.float32)], axis=0)
        pool[:, at : at + LANES] = jnp.transpose(rows).astype(jnp.bfloat16)
    tiles = pool.shape[1] // LANES
    total = translate(index, tile, matrix_ref, pool, tiles, lambda k: jnp.int16(k), 4)
    local_coeff = (total + own_ref[...]).astype(jnp.bfloat16)
    moment = jnp.dot(e_ref[...], local_coeff, preferred_element_type=jnp.float32)
    moment = moment.astype(jnp.bfloat16)
    for at, size in chunks_of(surface, 96):
        wide[pl.ds(at * 8, size * 8), :] = jnp.dot(
            d_ref[pl.ds(at * 8, size * 8), :], moment, preferred_element_type=jnp.float32
        )
        for c in range(8):
            out_ref[pl.ds(at, size), c * LANES : (c + 1) * LANES] = wide[
                pl.ds(at * 8 + c, size, stride=8), :
            ].astype(jnp.bfloat16)


def on_device(
    child_moments,
    upward_matrix,
    project_matrix,
    transfer_matrix,
    expand_matrix,
    downward_matrix,
    neighbour_list,
    ghost_map,
):
    surface = child_moments.shape[0]
    boxes = child_moments.shape[1] // 8
    coeff = project_matrix.shape[0]
    slots = ghost_map.shape[1]
    offsets = neighbour_list.shape[0]
    grp_count = lax.axis_size("grp")
    sub_count = lax.axis_size("sub")
    if boxes != LANES or sub_count & (sub_count - 1):
        raise ValueError("unsupported sizes")
    slot_lanes = -(-slots // LANES) * LANES
    packed, ghosts = pl.pallas_call(
        functools.partial(upward_kernel, 96),
        out_shape=(
            jax.ShapeDtypeStruct((coeff, boxes), jnp.bfloat16),
            jax.ShapeDtypeStruct((slots, coeff), jnp.bfloat16),
        ),
        in_specs=[VMEM] * 4,
        out_specs=(VMEM, VMEM),
        scratch_shapes=[
            pltpu.VMEM((-(-surface // LANES), surface * 8, LANES), jnp.float32),
            pltpu.VMEM((surface, boxes), jnp.bfloat16),
            pltpu.VMEM((1, slot_lanes), jnp.int32),
        ],
        compiler_params=pltpu.CompilerParams(vmem_limit_bytes=16 << 20),
        name="upward",
    )(
        child_moments,
        upward_matrix.reshape(surface * 8, surface),
        project_matrix,
        ghost_map,
    )
    send = jnp.broadcast_to(ghosts[None], (sub_count, slots, coeff)).reshape(sub_count * slots, coeff)
    received = lax.all_to_all(send, ("sub", "grp"), split_axis=0, concat_axis=0, tiled=True)
    own = packed
    hop = 1
    while hop < sub_count:
        other = lax.ppermute(own, "sub", [(i, i ^ hop) for i in range(sub_count)])
        own = jnp.concatenate([own, other], axis=1)
        hop *= 2
    me = lax.axis_index("sub").astype(jnp.int32).reshape(1, 1)
    own_part = pl.pallas_call(
        own_kernel,
        out_shape=jax.ShapeDtypeStruct((coeff, boxes), jnp.float32),
        in_specs=[SMEM] + [VMEM] * 3,
        out_specs=VMEM,
        scratch_shapes=[pltpu.VMEM((offsets, boxes), jnp.int32)] * 2,
        compiler_params=pltpu.CompilerParams(vmem_limit_bytes=16 << 20),
        cost_estimate=pl.CostEstimate(flops=2_000_000_000, bytes_accessed=1, transcendentals=0),
        name="own",
    )(me, neighbour_list, transfer_matrix, own)
    ghost_count = received.shape[0]
    ghost_lanes = -(-ghost_count // LANES) * LANES
    result = pl.pallas_call(
        functools.partial(ghost_kernel, sub_count * boxes),
        out_shape=jax.ShapeDtypeStruct((surface, 8 * boxes), jnp.bfloat16),
        in_specs=[VMEM] * 6,
        out_specs=VMEM,
        scratch_shapes=[pltpu.VMEM((offsets, boxes), jnp.int32)] * 2
        + [
            pltpu.VMEM((coeff, ghost_lanes), jnp.bfloat16),
            pltpu.VMEM((surface * 8, boxes), jnp.float32),
        ],
        compiler_params=pltpu.CompilerParams(vmem_limit_bytes=24 << 20),
        name="ghost_downward",
    )(
        neighbour_list,
        transfer_matrix,
        received,
        own_part,
        expand_matrix,
        downward_matrix.reshape(surface * 8, surface),
    )
    return result


def solution(mesh):
    return jax.shard_map(
        on_device,
        mesh=mesh,
        in_specs=(
            P(None, ("grp", "sub")),
            P(),
            P(),
            P(),
            P(),
            P(),
            P(None, ("grp", "sub")),
            P(("grp", "sub"), None),
        ),
        out_specs=P(None, ("grp", "sub")),
        check_vma=False,
    )
```

```python
import functools

import jax
import jax.numpy as jnp
from jax import lax
from jax.experimental import pallas as pl
from jax.experimental.pallas import tpu as pltpu
from jax.sharding import PartitionSpec as P

LANES = 128
VMEM = pl.BlockSpec(memory_space=pltpu.VMEM)
HBM = pl.BlockSpec(memory_space=pltpu.HBM)
SMEM = pl.BlockSpec(memory_space=pltpu.SMEM)


def lane_gather(values, lanes):
    numbers = lax.GatherDimensionNumbers(
        offset_dims=(),
        collapsed_slice_dims=(1,),
        start_index_map=(1,),
        operand_batching_dims=(0,),
        start_indices_batching_dims=(0,),
    )
    return lax.gather(
        values,
        lanes[..., None],
        numbers,
        slice_sizes=(1, 1),
        mode=lax.GatherScatterMode.PROMISE_IN_BOUNDS,
    )


def chunks_of(total, size):
    return [(at, min(size, total - at)) for at in range(0, total, size)]


def upward_kernel(x_hbm, u_hbm, p_hbm, map_hbm, packed_ref, ghost_ref, x_ref, u_ref, p_ref, map_ref, slots, wide, parent, sems):
    surface = x_ref.shape[0]
    coeff = p_ref.shape[0]
    used = map_hbm.shape[1]
    chunks = chunks_of(surface, 96)
    x_copy = pltpu.make_async_copy(x_hbm, x_ref, sems.at[0])
    x_copy.start()
    u_copies = []
    for n, (at, size) in enumerate(chunks):
        rows = pl.ds(at * 8, size * 8)
        u_copies.append(pltpu.make_async_copy(u_hbm.at[rows, :], u_ref.at[rows, :], sems.at[3 + n]))
        u_copies[-1].start()
    p_copy = pltpu.make_async_copy(p_hbm, p_ref, sems.at[1])
    p_copy.start()
    slots[...] = jnp.full(slots.shape, LANES, jnp.int32)
    map_copy = pltpu.make_async_copy(map_hbm, map_ref, sems.at[2])
    map_copy.start()
    x_copy.wait()
    for n, (at, size) in enumerate(chunks):
        u_copies[n].wait()
        for m, (left, width) in enumerate(chunks_of(surface, LANES)):
            wide[m, pl.ds(at * 8, size * 8), 0:width] = u_ref[
                pl.ds(at * 8, size * 8), left : left + width
            ].astype(jnp.float32)
        total = jnp.zeros((size, LANES), jnp.float32)
        for c in range(8):
            matrix = jnp.concatenate(
                [
                    wide.at[m][pl.ds(at * 8 + c, size, stride=8), :].astype(jnp.bfloat16)[:, :width]
                    for m, (_, width) in enumerate(chunks_of(surface, LANES))
                ],
                axis=1,
            )
            total += jnp.dot(
                matrix,
                x_ref[:, c * LANES : (c + 1) * LANES],
                preferred_element_type=jnp.float32,
            )
        parent[pl.ds(at, size), :] = total.astype(jnp.bfloat16)
    p_copy.wait()
    map_copy.wait()
    slots[:, 0:used] = map_ref[...]
    packed = jnp.dot(p_ref[...], parent[...], preferred_element_type=jnp.float32)
    packed = packed.astype(jnp.bfloat16)
    packed_ref[...] = packed
    for at in range(0, slots.shape[1], LANES):
        ids = jnp.broadcast_to(slots[:, at : at + LANES], (coeff, LANES))
        taken = lane_gather(packed, (ids & (LANES - 1)).astype(jnp.int16)).astype(jnp.float32)
        taken = jnp.where(ids < LANES, taken, 0.0)
        rows = jnp.transpose(taken).astype(jnp.bfloat16)
        keep = min(LANES, used - at)
        ghost_ref[at : at + keep, :] = rows[:keep, :]


def spread(row, rows):
    return jnp.broadcast_to(row, (rows, LANES))


def pick_lanes(code, pool_ref, coeff):
    tiles = pool_ref.shape[1] // LANES
    lanes = spread(code & (LANES - 1), coeff).astype(jnp.int16)
    place = spread(code >> 7, coeff).astype(jnp.int16)
    out = jnp.zeros((coeff, LANES), jnp.bfloat16)
    if tiles <= 8:
        for k in range(tiles):
            got = lane_gather(pool_ref[:, k * LANES : (k + 1) * LANES], lanes)
            out = jnp.where(place == jnp.int16(k), got, out)
        return out

    def one(k, out):
        got = lane_gather(pool_ref[:, pl.ds(pl.multiple_of(k * LANES, LANES), LANES)], lanes)
        return jnp.where(place == k.astype(jnp.int16), got, out)

    return lax.fori_loop(0, tiles, one, out)


def pick_pair(codes, stack_ref, coeff, count):
    runs = stack_ref.shape[0] // coeff
    wide = 2 * LANES
    marks = []
    for code in codes:
        low = spread(jnp.where(code < 0, -1, code & (wide - 1)), wide).astype(jnp.int16)
        marks.append(
            jnp.where(count == low, jnp.bfloat16(1), jnp.bfloat16(0))
        )
    got = jnp.dot(
        stack_ref[...], jnp.concatenate(marks, axis=1), preferred_element_type=jnp.float32
    )
    out = []
    for n, code in enumerate(codes):
        run = spread(code >> 8, coeff)
        best = got[0:coeff, n * LANES : (n + 1) * LANES]
        for k in range(1, runs):
            best = jnp.where(run == k, got[k * coeff : (k + 1) * coeff, n * LANES : (n + 1) * LANES], best)
        out.append(best.astype(jnp.bfloat16))
    return out


GROUP = 80
BY_DOT = 46


def translate(code_ref, matrix_ref, pool_ref, stack_ref, picked):
    coeff = pool_ref.shape[0]
    offsets = code_ref.shape[0]
    small = pool_ref.shape[1] // LANES <= 8
    if small:
        for k in range(stack_ref.shape[0] // coeff):
            left = k * 2 * LANES
            part = pool_ref[:, left : min(left + 2 * LANES, pool_ref.shape[1])]
            if part.shape[1] < 2 * LANES:
                part = jnp.concatenate([part, jnp.zeros((coeff, LANES), jnp.bfloat16)], axis=1)
            stack_ref[k * coeff : (k + 1) * coeff, :] = part
    count_in_run = lax.broadcasted_iota(jnp.int32, (2 * LANES, LANES), 0).astype(jnp.int16)

    def picks(at, count):
        by_dot = min(BY_DOT, count) // 2 * 2 if small else 0
        done = 0
        for n in range(count - by_dot + by_dot // 2):
            total = count - by_dot + by_dot // 2
            pairs = by_dot // 2
            if (n + 1) * pairs // total > n * pairs // total:
                rows = [code_ref[pl.ds(at + done + m, 1), :] for m in (0, 1)]
                keep(at + done, pick_pair(rows, stack_ref, coeff, count_in_run))
                done += 2
            else:
                keep(at + done, [pick_lanes(code_ref[pl.ds(at + done, 1), :], pool_ref, coeff)])
                done += 1

    def keep(at, parts):
        for n, part in enumerate(parts):
            picked[pl.ds(pl.multiple_of((at + n) * coeff, coeff), coeff), :] = part

    def product(at, count):
        start = pl.multiple_of(at * coeff, LANES)
        return jnp.dot(
            matrix_ref[:, pl.ds(start, count * coeff)],
            picked[pl.ds(start, count * coeff), :],
            preferred_element_type=jnp.float32,
        )

    trips = offsets // GROUP
    rest = offsets - trips * GROUP
    picks(0, GROUP)

    def body(i, total):
        total += product((i - 1) * GROUP, GROUP)
        picks(i * GROUP, GROUP)
        return total

    total = lax.fori_loop(1, trips, body, jnp.zeros((coeff, LANES), jnp.float32))
    total += product((trips - 1) * GROUP, GROUP)
    if rest:
        picks(trips * GROUP, rest)
        total += product(trips * GROUP, rest)
    return total


def translate_scratch(offsets, coeff, lanes):
    return [
        pltpu.VMEM((offsets, LANES), jnp.int32),
        pltpu.VMEM((-(-lanes // (2 * LANES)) * coeff, 2 * LANES), jnp.bfloat16),
        pltpu.VMEM((offsets * coeff, LANES), jnp.bfloat16),
    ]


def own_kernel(me_ref, list_ref, matrix_ref, pool_ref, out_ref, code, stack, picked):
    me = me_ref[0, 0]
    lists = list_ref[...]
    code[...] = jnp.where(lists < pool_ref.shape[1], lists ^ (me * LANES), -1)
    out_ref[...] = translate(code, matrix_ref, pool_ref, stack, picked)


def fold_kernel(e_ref, d_ref, down_ref):
    down_ref[...] = lax.dot_general(
        d_ref[...], e_ref[...], (((1,), (1,)), ((), ())), preferred_element_type=jnp.float32
    ).astype(jnp.bfloat16)


def ghost_kernel(own_boxes, list_ref, matrix_ref, rows_ref, own_ref, down_ref, out_ref, code, stack, picked, pool, wide):
    coeff = matrix_ref.shape[0]
    surface = out_ref.shape[0]
    slots = rows_ref.shape[0]
    lists = list_ref[...] - own_boxes
    code[...] = jnp.where(lists < slots, lists, -1)
    for at, size in chunks_of(slots, LANES):
        rows = rows_ref[at : at + size, :].astype(jnp.float32)
        if size < LANES:
            rows = jnp.concatenate([rows, jnp.zeros((LANES - size, coeff), jnp.float32)], axis=0)
        pool[:, at : at + LANES] = jnp.transpose(rows).astype(jnp.bfloat16)
    total = translate(code, matrix_ref, pool, stack, picked)
    local_coeff = (total + own_ref[...]).astype(jnp.bfloat16)
    for at, size in chunks_of(surface, 96):
        wide[pl.ds(at * 8, size * 8), :] = jnp.dot(
            down_ref[pl.ds(at * 8, size * 8), :], local_coeff, preferred_element_type=jnp.float32
        )
        for c in range(8):
            out_ref[pl.ds(at, size), c * LANES : (c + 1) * LANES] = wide[
                pl.ds(at * 8 + c, size, stride=8), :
            ].astype(jnp.bfloat16)


def on_device(
    child_moments,
    upward_matrix,
    project_matrix,
    transfer_matrix,
    expand_matrix,
    downward_matrix,
    neighbour_list,
    ghost_map,
):
    surface = child_moments.shape[0]
    boxes = child_moments.shape[1] // 8
    coeff = project_matrix.shape[0]
    slots = ghost_map.shape[1]
    offsets = neighbour_list.shape[0]
    grp_count = lax.axis_size("grp")
    sub_count = lax.axis_size("sub")
    if boxes != LANES or sub_count & (sub_count - 1):
        raise ValueError("unsupported sizes")
    slot_lanes = -(-slots // LANES) * LANES
    lane_tiles = -(-surface // LANES)
    packed, ghosts = pl.pallas_call(
        upward_kernel,
        out_shape=(
            jax.ShapeDtypeStruct((coeff, boxes), jnp.bfloat16),
            jax.ShapeDtypeStruct((slots, coeff), jnp.bfloat16),
        ),
        in_specs=[HBM] * 4,
        out_specs=(VMEM, VMEM),
        scratch_shapes=[
            pltpu.VMEM(child_moments.shape, jnp.bfloat16),
            pltpu.VMEM((surface * 8, surface), jnp.bfloat16),
            pltpu.VMEM(project_matrix.shape, jnp.bfloat16),
            pltpu.VMEM(ghost_map.shape, jnp.int32),
            pltpu.VMEM((1, slot_lanes), jnp.int32),
            pltpu.VMEM((lane_tiles, surface * 8, LANES), jnp.float32),
            pltpu.VMEM((surface, boxes), jnp.bfloat16),
            pltpu.SemaphoreType.DMA((3 + len(chunks_of(surface, 96)),)),
        ],
        compiler_params=pltpu.CompilerParams(vmem_limit_bytes=40000 << 10),
        cost_estimate=pl.CostEstimate(flops=500_000_000, bytes_accessed=3_000_000, transcendentals=0),
        name="upward",
    )(
        *(
            pltpu.with_memory_space_constraint(a, pltpu.HBM)
            for a in (child_moments, upward_matrix.reshape(surface * 8, surface), project_matrix, ghost_map)
        )
    )
    send = jnp.broadcast_to(ghosts[None], (sub_count, slots, coeff)).reshape(sub_count * slots, coeff)
    received = lax.all_to_all(send, ("sub", "grp"), split_axis=0, concat_axis=0, tiled=True)
    own = packed
    hop = 1
    while hop < sub_count:
        other = lax.ppermute(own, "sub", [(i, i ^ hop) for i in range(sub_count)])
        own = jnp.concatenate([own, other], axis=1)
        hop *= 2
    me = lax.axis_index("sub").astype(jnp.int32).reshape(1, 1)
    own_part = pl.pallas_call(
        own_kernel,
        out_shape=jax.ShapeDtypeStruct((coeff, boxes), jnp.float32),
        in_specs=[SMEM] + [VMEM] * 3,
        out_specs=VMEM,
        scratch_shapes=translate_scratch(offsets, coeff, own.shape[1]),
        compiler_params=pltpu.CompilerParams(vmem_limit_bytes=20 << 20),
        cost_estimate=pl.CostEstimate(flops=3_000_000_000, bytes_accessed=1, transcendentals=0),
        name="own",
    )(me, neighbour_list, transfer_matrix, own)
    down = pl.pallas_call(
        fold_kernel,
        out_shape=jax.ShapeDtypeStruct((surface * 8, coeff), jnp.bfloat16),
        in_specs=[VMEM] * 2,
        out_specs=VMEM,
        compiler_params=pltpu.CompilerParams(vmem_limit_bytes=8 << 20),
        cost_estimate=pl.CostEstimate(flops=500_000_000, bytes_accessed=1, transcendentals=0),
        name="fold",
    )(jnp.transpose(expand_matrix), downward_matrix.reshape(surface * 8, surface))
    ghost_count = received.shape[0]
    ghost_lanes = -(-ghost_count // LANES) * LANES
    result = pl.pallas_call(
        functools.partial(ghost_kernel, sub_count * boxes),
        out_shape=jax.ShapeDtypeStruct((surface, 8 * boxes), jnp.bfloat16),
        in_specs=[VMEM] * 5,
        out_specs=VMEM,
        scratch_shapes=translate_scratch(offsets, coeff, ghost_lanes)
        + [
            pltpu.VMEM((coeff, ghost_lanes), jnp.bfloat16),
            pltpu.VMEM((surface * 8, boxes), jnp.float32),
        ],
        compiler_params=pltpu.CompilerParams(vmem_limit_bytes=20 << 20),
        name="ghost_downward",
    )(neighbour_list, transfer_matrix, received, own_part, down)
    return result


def solution(mesh):
    return jax.shard_map(
        on_device,
        mesh=mesh,
        in_specs=(
            P(None, ("grp", "sub")),
            P(),
            P(),
            P(),
            P(),
            P(),
            P(None, ("grp", "sub")),
            P(("grp", "sub"), None),
        ),
        out_specs=P(None, ("grp", "sub")),
        check_vma=False,
    )
```

```python
import functools

import jax
import jax.numpy as jnp
from jax import lax
from jax.experimental import pallas as pl
from jax.experimental.pallas import tpu as pltpu
from jax.sharding import PartitionSpec as P

LANES = 128
ROWS = 8
VMEM = pl.BlockSpec(memory_space=pltpu.VMEM)
HBM = pl.BlockSpec(memory_space=pltpu.HBM)
SMEM = pl.BlockSpec(memory_space=pltpu.SMEM)


def lane_gather(values, lanes):
    numbers = lax.GatherDimensionNumbers(
        offset_dims=(),
        collapsed_slice_dims=(1,),
        start_index_map=(1,),
        operand_batching_dims=(0,),
        start_indices_batching_dims=(0,),
    )
    return lax.gather(
        values,
        lanes[..., None],
        numbers,
        slice_sizes=(1, 1),
        mode=lax.GatherScatterMode.PROMISE_IN_BOUNDS,
    )


def chunks_of(total, size):
    return [(at, min(size, total - at)) for at in range(0, total, size)]


def upward_kernel(
    groups, x_hbm, u_hbm, p_hbm, map_hbm, packed_ref, ghost_ref,
    x_ref, u_ref, p_ref, map_ref, slots, wide, parent, taken_rows, sems
):
    surface = x_ref.shape[0]
    coeff = p_ref.shape[0]
    used = map_hbm.shape[1]
    chunks = chunks_of(surface, 96)
    x_copy = pltpu.make_async_copy(x_hbm, x_ref, sems.at[0])
    x_copy.start()
    u_copies = []
    for n, (at, size) in enumerate(chunks):
        rows = pl.ds(at * 8, size * 8)
        u_copies.append(pltpu.make_async_copy(u_hbm.at[rows, :], u_ref.at[rows, :], sems.at[3 + n]))
        u_copies[-1].start()
    p_copy = pltpu.make_async_copy(p_hbm, p_ref, sems.at[1])
    p_copy.start()
    slots[...] = jnp.full(slots.shape, LANES, jnp.int32)
    map_copy = pltpu.make_async_copy(map_hbm, map_ref, sems.at[2])
    map_copy.start()
    x_copy.wait()
    for n, (at, size) in enumerate(chunks):
        u_copies[n].wait()
        for m, (left, width) in enumerate(chunks_of(surface, LANES)):
            wide[m, pl.ds(at * 8, size * 8), 0:width] = u_ref[
                pl.ds(at * 8, size * 8), left : left + width
            ].astype(jnp.float32)
        total = jnp.zeros((size, LANES), jnp.float32)
        for c in range(8):
            matrix = jnp.concatenate(
                [
                    wide.at[m][pl.ds(at * 8 + c, size, stride=8), :].astype(jnp.bfloat16)[:, :width]
                    for m, (_, width) in enumerate(chunks_of(surface, LANES))
                ],
                axis=1,
            )
            total += jnp.dot(
                matrix,
                x_ref[:, c * LANES : (c + 1) * LANES],
                preferred_element_type=jnp.float32,
            )
        parent[pl.ds(at, size), :] = total.astype(jnp.bfloat16)
    p_copy.wait()
    map_copy.wait()
    slots[:, 0:used] = map_ref[...]
    packed = jnp.dot(p_ref[...], parent[...], preferred_element_type=jnp.float32)
    packed = packed.astype(jnp.bfloat16)
    packed_ref[...] = packed
    for at in range(0, slots.shape[1], LANES):
        ids = jnp.broadcast_to(slots[:, at : at + LANES], (coeff, LANES))
        taken = lane_gather(packed, (ids & (LANES - 1)).astype(jnp.int16)).astype(jnp.float32)
        taken = jnp.where(ids < LANES, taken, 0.0)
        taken_rows[at : at + LANES, :] = jnp.transpose(taken)
    width = used // groups
    copies = ghost_ref.shape[0] // (groups * ROWS)
    for g in range(groups):
        first = taken_rows[g * width : g * width + ROWS, :]
        second = taken_rows[g * width + ROWS : g * width + 2 * ROWS, :]
        rows = jnp.concatenate([first, second], axis=1).astype(jnp.bfloat16)
        for n in range(copies):
            at = (n * groups + g) * ROWS
            ghost_ref[at : at + ROWS, :] = rows


def spread(row, rows):
    return jnp.broadcast_to(row, (rows, LANES))


def pick_lanes(code, pool_ref, coeff):
    tiles = pool_ref.shape[1] // LANES
    lanes = spread(code & (LANES - 1), coeff).astype(jnp.int16)
    place = spread(code >> 7, coeff).astype(jnp.int16)
    out = jnp.zeros((coeff, LANES), jnp.bfloat16)
    if tiles <= 8:
        for k in range(tiles):
            got = lane_gather(pool_ref[:, k * LANES : (k + 1) * LANES], lanes)
            out = jnp.where(place == jnp.int16(k), got, out)
        return out

    def one(k, out):
        got = lane_gather(pool_ref[:, pl.ds(pl.multiple_of(k * LANES, LANES), LANES)], lanes)
        return jnp.where(place == k.astype(jnp.int16), got, out)

    return lax.fori_loop(0, tiles, one, out)


def pick_pair(codes, stack_ref, coeff, count):
    runs = stack_ref.shape[0] // coeff
    wide = 2 * LANES
    marks = []
    for code in codes:
        low = spread(jnp.where(code < 0, -1, code & (wide - 1)), wide).astype(jnp.int16)
        marks.append(
            jnp.where(count == low, jnp.bfloat16(1), jnp.bfloat16(0))
        )
    got = jnp.dot(
        stack_ref[...], jnp.concatenate(marks, axis=1), preferred_element_type=jnp.float32
    )
    out = []
    for n, code in enumerate(codes):
        run = spread(code >> 8, coeff)
        best = got[0:coeff, n * LANES : (n + 1) * LANES]
        for k in range(1, runs):
            best = jnp.where(run == k, got[k * coeff : (k + 1) * coeff, n * LANES : (n + 1) * LANES], best)
        out.append(best.astype(jnp.bfloat16))
    return out


GROUP = 80
BY_DOT = 46


def translate(code_ref, matrix_ref, pool_ref, stack_ref, picked):
    coeff = pool_ref.shape[0]
    offsets = code_ref.shape[0]
    small = pool_ref.shape[1] // LANES <= 8
    if small:
        for k in range(stack_ref.shape[0] // coeff):
            left = k * 2 * LANES
            part = pool_ref[:, left : min(left + 2 * LANES, pool_ref.shape[1])]
            if part.shape[1] < 2 * LANES:
                part = jnp.concatenate([part, jnp.zeros((coeff, LANES), jnp.bfloat16)], axis=1)
            stack_ref[k * coeff : (k + 1) * coeff, :] = part
    count_in_run = lax.broadcasted_iota(jnp.int32, (2 * LANES, LANES), 0).astype(jnp.int16)

    def picks(at, count):
        by_dot = min(BY_DOT, count) // 2 * 2 if small else 0
        done = 0
        for n in range(count - by_dot + by_dot // 2):
            total = count - by_dot + by_dot // 2
            pairs = by_dot // 2
            if (n + 1) * pairs // total > n * pairs // total:
                rows = [code_ref[pl.ds(at + done + m, 1), :] for m in (0, 1)]
                keep(at + done, pick_pair(rows, stack_ref, coeff, count_in_run))
                done += 2
            else:
                keep(at + done, [pick_lanes(code_ref[pl.ds(at + done, 1), :], pool_ref, coeff)])
                done += 1

    def keep(at, parts):
        for n, part in enumerate(parts):
            picked[pl.ds(pl.multiple_of((at + n) * coeff, coeff), coeff), :] = part

    def product(at, count):
        start = pl.multiple_of(at * coeff, LANES)
        return jnp.dot(
            matrix_ref[:, pl.ds(start, count * coeff)],
            picked[pl.ds(start, count * coeff), :],
            preferred_element_type=jnp.float32,
        )

    trips = offsets // GROUP
    rest = offsets - trips * GROUP
    picks(0, GROUP)

    def body(i, total):
        total += product((i - 1) * GROUP, GROUP)
        picks(i * GROUP, GROUP)
        return total

    total = lax.fori_loop(1, trips, body, jnp.zeros((coeff, LANES), jnp.float32))
    total += product((trips - 1) * GROUP, GROUP)
    if rest:
        picks(trips * GROUP, rest)
        total += product(trips * GROUP, rest)
    return total


def translate_scratch(offsets, coeff, lanes):
    return [
        pltpu.VMEM((offsets, LANES), jnp.int32),
        pltpu.VMEM((-(-lanes // (2 * LANES)) * coeff, 2 * LANES), jnp.bfloat16),
        pltpu.VMEM((offsets * coeff, LANES), jnp.bfloat16),
    ]


def own_kernel(
    me_ref, list_ref, matrix_ref, pool_ref, e_ref, d_hbm, out_ref, down_ref, code, stack, picked, d_ref, sem
):
    d_copy = pltpu.make_async_copy(d_hbm, d_ref, sem)
    d_copy.start()
    me = me_ref[0, 0]
    lists = list_ref[...]
    code[...] = jnp.where(lists < pool_ref.shape[1], lists ^ (me * LANES), -1)
    out_ref[...] = translate(code, matrix_ref, pool_ref, stack, picked)
    d_copy.wait()
    down_ref[...] = lax.dot_general(
        d_ref[...], e_ref[...], (((1,), (1,)), ((), ())), preferred_element_type=jnp.float32
    ).astype(jnp.bfloat16)


def ghost_kernel(
    own_boxes, width, list_ref, matrix_ref, rows_ref, own_ref, down_ref, out_ref, code, stack, picked, pool, extra, wide
):
    coeff = matrix_ref.shape[0]
    surface = out_ref.shape[0]
    lanes = rows_ref.shape[0]
    senders = lanes // ROWS
    more = width - ROWS
    lists = list_ref[...] - own_boxes
    sender = ((lists.astype(jnp.float32) + 0.5) * (1.0 / width)).astype(jnp.int32)
    slot = lists - sender * width
    place = jnp.where(
        slot < ROWS, sender * ROWS + slot, lanes + sender * more + slot - ROWS
    )
    code[...] = jnp.where((lists >= 0) & (lists < senders * width), place, -1)
    for at in range(0, lanes, LANES):
        turned = jnp.transpose(rows_ref[at : at + LANES, :].astype(jnp.float32)).astype(jnp.bfloat16)
        pool[:, at : at + LANES] = turned[0:coeff, :]
        extra[:, at : at + LANES] = turned[coeff : 2 * coeff, :]
    for at in range(0, pool.shape[1] - lanes, LANES):
        m = lax.broadcasted_iota(jnp.int32, (coeff, LANES), 1) + at
        source = (m >> (more.bit_length() - 1)) * ROWS + (m & (more - 1))
        lane, tile = (source & (LANES - 1)).astype(jnp.int16), (source >> 7).astype(jnp.int16)
        got = jnp.zeros((coeff, LANES), jnp.bfloat16)
        first = at // more * ROWS // LANES
        for k in range(first, min(first + LANES // more * ROWS // LANES, lanes // LANES)):
            part = lane_gather(extra[:, k * LANES : (k + 1) * LANES], lane)
            got = jnp.where(tile == jnp.int16(k), part, got)
        pool[:, lanes + at : lanes + at + LANES] = got
    total = translate(code, matrix_ref, pool, stack, picked)
    local_coeff = (total + own_ref[...]).astype(jnp.bfloat16)
    for at, size in chunks_of(surface, 96):
        wide[pl.ds(at * 8, size * 8), :] = jnp.dot(
            down_ref[pl.ds(at * 8, size * 8), :], local_coeff, preferred_element_type=jnp.float32
        )
        for c in range(8):
            out_ref[pl.ds(at, size), c * LANES : (c + 1) * LANES] = wide[
                pl.ds(at * 8 + c, size, stride=8), :
            ].astype(jnp.bfloat16)


def on_device(
    child_moments,
    upward_matrix,
    project_matrix,
    transfer_matrix,
    expand_matrix,
    downward_matrix,
    neighbour_list,
    ghost_map,
):
    surface = child_moments.shape[0]
    boxes = child_moments.shape[1] // 8
    coeff = project_matrix.shape[0]
    slots = ghost_map.shape[1]
    offsets = neighbour_list.shape[0]
    grp_count = lax.axis_size("grp")
    sub_count = lax.axis_size("sub")
    if boxes != LANES or sub_count & (sub_count - 1):
        raise ValueError("unsupported sizes")
    slot_lanes = -(-(slots + ROWS) // LANES) * LANES
    width = slots // grp_count
    more = width - ROWS
    if 2 * coeff != LANES or not 0 < more <= ROWS or more & (more - 1):
        raise ValueError("unsupported sizes")
    lane_tiles = -(-surface // LANES)
    packed, send = pl.pallas_call(
        functools.partial(upward_kernel, grp_count),
        out_shape=(
            jax.ShapeDtypeStruct((coeff, boxes), jnp.bfloat16),
            jax.ShapeDtypeStruct((sub_count * grp_count * ROWS, LANES), jnp.bfloat16),
        ),
        in_specs=[HBM] * 4,
        out_specs=(VMEM, VMEM),
        scratch_shapes=[
            pltpu.VMEM(child_moments.shape, jnp.bfloat16),
            pltpu.VMEM((surface * 8, surface), jnp.bfloat16),
            pltpu.VMEM(project_matrix.shape, jnp.bfloat16),
            pltpu.VMEM(ghost_map.shape, jnp.int32),
            pltpu.VMEM((1, slot_lanes), jnp.int32),
            pltpu.VMEM((lane_tiles, surface * 8, LANES), jnp.float32),
            pltpu.VMEM((surface, boxes), jnp.bfloat16),
            pltpu.VMEM((slot_lanes, coeff), jnp.float32),
            pltpu.SemaphoreType.DMA((3 + len(chunks_of(surface, 96)),)),
        ],
        compiler_params=pltpu.CompilerParams(vmem_limit_bytes=40000 << 10),
        cost_estimate=pl.CostEstimate(flops=500_000_000, bytes_accessed=3_000_000, transcendentals=0),
        name="upward",
    )(
        *(
            pltpu.with_memory_space_constraint(a, pltpu.HBM)
            for a in (
                child_moments,
                upward_matrix.reshape(surface * 8, surface),
                project_matrix,
                ghost_map,
            )
        )
    )
    received = lax.all_to_all(send, ("sub", "grp"), split_axis=0, concat_axis=0, tiled=True)
    own = packed
    hop = 1
    while hop < sub_count:
        other = lax.ppermute(own, "sub", [(i, i ^ hop) for i in range(sub_count)])
        own = jnp.concatenate([own, other], axis=1)
        hop *= 2
    me = lax.axis_index("sub").astype(jnp.int32).reshape(1, 1)
    own_part, down = pl.pallas_call(
        own_kernel,
        out_shape=(
            jax.ShapeDtypeStruct((coeff, boxes), jnp.float32),
            jax.ShapeDtypeStruct((surface * 8, coeff), jnp.bfloat16),
        ),
        in_specs=[SMEM] + [VMEM] * 4 + [HBM],
        out_specs=(VMEM, VMEM),
        scratch_shapes=translate_scratch(offsets, coeff, own.shape[1])
        + [
            pltpu.VMEM((surface * 8, surface), jnp.bfloat16),
            pltpu.SemaphoreType.DMA(()),
        ],
        compiler_params=pltpu.CompilerParams(vmem_limit_bytes=24 << 20),
        cost_estimate=pl.CostEstimate(flops=3_000_000_000, bytes_accessed=1, transcendentals=0),
        name="own",
    )(
        me,
        neighbour_list,
        transfer_matrix,
        own,
        jnp.transpose(expand_matrix),
        pltpu.with_memory_space_constraint(downward_matrix.reshape(surface * 8, surface), pltpu.HBM),
    )
    sent_lanes = received.shape[0]
    ghost_lanes = sent_lanes + -(-(sent_lanes // ROWS * more) // LANES) * LANES
    result = pl.pallas_call(
        functools.partial(ghost_kernel, sub_count * boxes, width),
        out_shape=jax.ShapeDtypeStruct((surface, 8 * boxes), jnp.bfloat16),
        in_specs=[VMEM] * 5,
        out_specs=VMEM,
        scratch_shapes=translate_scratch(offsets, coeff, ghost_lanes)
        + [
            pltpu.VMEM((coeff, ghost_lanes), jnp.bfloat16),
            pltpu.VMEM((coeff, sent_lanes), jnp.bfloat16),
            pltpu.VMEM((surface * 8, boxes), jnp.float32),
        ],
        compiler_params=pltpu.CompilerParams(vmem_limit_bytes=20 << 20),
        name="ghost_downward",
    )(neighbour_list, transfer_matrix, received, own_part, down)
    return result


def solution(mesh):
    return jax.shard_map(
        on_device,
        mesh=mesh,
        in_specs=(
            P(None, ("grp", "sub")),
            P(),
            P(),
            P(),
            P(),
            P(),
            P(None, ("grp", "sub")),
            P(("grp", "sub"), None),
        ),
        out_specs=P(None, ("grp", "sub")),
        check_vma=False,
    )
```

```python
import functools

import jax
import jax.numpy as jnp
from jax import lax
from jax.experimental import pallas as pl
from jax.experimental.pallas import tpu as pltpu
from jax.sharding import PartitionSpec as P


LANES = 128
ROWS = 8
VMEM = pl.BlockSpec(memory_space=pltpu.VMEM)
HBM = pl.BlockSpec(memory_space=pltpu.HBM)
SMEM = pl.BlockSpec(memory_space=pltpu.SMEM)


def lane_gather(values, lanes):
    numbers = lax.GatherDimensionNumbers(
        offset_dims=(),
        collapsed_slice_dims=(1,),
        start_index_map=(1,),
        operand_batching_dims=(0,),
        start_indices_batching_dims=(0,),
    )
    return lax.gather(
        values,
        lanes[..., None],
        numbers,
        slice_sizes=(1, 1),
        mode=lax.GatherScatterMode.PROMISE_IN_BOUNDS,
    )


def chunks_of(total, size):
    return [(at, min(size, total - at)) for at in range(0, total, size)]


def upward_kernel(
    groups, x_hbm, u_hbm, p_hbm, map_hbm, packed_ref, ghost_ref,
    x_ref, u_ref, p_ref, map_ref, slots, wide, parent, taken_rows, sems
):
    surface = x_ref.shape[0]
    coeff = p_ref.shape[0]
    used = map_hbm.shape[1]
    chunks = chunks_of(surface, 96)
    u_copies = []
    for n, (at, size) in enumerate(chunks):
        rows = pl.ds(at * 8, size * 8)
        u_copies.append(pltpu.make_async_copy(u_hbm.at[rows, :], u_ref.at[rows, :], sems.at[3 + n]))
        u_copies[-1].start()
    x_copy = pltpu.make_async_copy(x_hbm, x_ref, sems.at[0])
    x_copy.start()
    p_copy = pltpu.make_async_copy(p_hbm, p_ref, sems.at[1])
    p_copy.start()
    slots[...] = jnp.full(slots.shape, LANES, jnp.int32)
    map_copy = pltpu.make_async_copy(map_hbm, map_ref, sems.at[2])
    map_copy.start()
    lane_chunks = list(enumerate(chunks_of(surface, LANES)))
    for n, (at, size) in enumerate(chunks):
        u_copies[n].wait()
        for m, (left, width) in lane_chunks:
            wide[m, pl.ds(at * 8, size * 8), 0:width] = u_ref[
                pl.ds(at * 8, size * 8), left : left + width
            ].astype(jnp.float32)
    x_copy.wait()
    total = jnp.zeros((surface, LANES), jnp.float32)
    for c in range(8):
        matrix = jnp.concatenate(
            [wide.at[m][pl.ds(c, surface, stride=8), :].astype(jnp.bfloat16)[:, :width] for m, (_, width) in lane_chunks],
            axis=1,
        )
        total += jnp.dot(
            matrix, x_ref[:, c * LANES : (c + 1) * LANES], preferred_element_type=jnp.float32
        )
    parent[...] = total.astype(jnp.bfloat16)
    p_copy.wait()
    map_copy.wait()
    slots[:, 0:used] = map_ref[...]
    packed = jnp.dot(p_ref[...], parent[...], preferred_element_type=jnp.float32)
    packed = packed.astype(jnp.bfloat16)
    packed_ref[...] = packed
    for at in range(0, slots.shape[1], LANES):
        ids = jnp.broadcast_to(slots[:, at : at + LANES], (coeff, LANES))
        taken = lane_gather(packed, (ids & (LANES - 1)).astype(jnp.int16)).astype(jnp.float32)
        taken = jnp.where(ids < LANES, taken, 0.0)
        taken_rows[at : at + LANES, :] = jnp.transpose(taken)
    width = used // groups
    copies = ghost_ref.shape[0] // (groups * ROWS)
    for g in range(groups):
        first = taken_rows[g * width : g * width + ROWS, :]
        second = taken_rows[g * width + ROWS : g * width + 2 * ROWS, :]
        rows = jnp.concatenate([first, second], axis=1).astype(jnp.bfloat16)
        for n in range(copies):
            at = (n * groups + g) * ROWS
            ghost_ref[at : at + ROWS, :] = rows


def spread(row, rows):
    return jnp.broadcast_to(row, (rows, LANES))


def pick_lanes(code, pool_ref, coeff):
    tiles = pool_ref.shape[1] // LANES
    lanes = spread(code & (LANES - 1), coeff).astype(jnp.int16)
    place = spread(code >> 7, coeff).astype(jnp.int16)
    out = jnp.zeros((coeff, LANES), jnp.bfloat16)
    if tiles <= 8:
        for k in range(tiles):
            got = lane_gather(pool_ref[:, k * LANES : (k + 1) * LANES], lanes)
            out = jnp.where(place == jnp.int16(k), got, out)
        return out

    def one(k, out):
        got = lane_gather(pool_ref[:, pl.ds(pl.multiple_of(k * LANES, LANES), LANES)], lanes)
        return jnp.where(place == k.astype(jnp.int16), got, out)

    return lax.fori_loop(0, tiles, one, out)


def pick_pair(codes, stack_ref, coeff, count):
    runs = stack_ref.shape[0] // coeff
    wide = 2 * LANES
    marks = []
    for code in codes:
        low = spread(jnp.where(code < 0, -1, code & (wide - 1)), wide).astype(jnp.int16)
        marks.append(
            jnp.where(count == low, jnp.bfloat16(1), jnp.bfloat16(0))
        )
    got = jnp.dot(
        stack_ref[...], jnp.concatenate(marks, axis=1), preferred_element_type=jnp.float32
    )
    out = []
    for n, code in enumerate(codes):
        run = spread(code >> 8, coeff)
        best = got[0:coeff, n * LANES : (n + 1) * LANES]
        for k in range(1, runs):
            best = jnp.where(run == k, got[k * coeff : (k + 1) * coeff, n * LANES : (n + 1) * LANES], best)
        out.append(best.astype(jnp.bfloat16))
    return out


OWN_GROUP = (80, 58)
GHOST_GROUP = (158, 108)


def translate(group, code_ref, matrix_ref, pool_ref, stack_ref, picked):
    GROUP, BY_DOT = group
    coeff = pool_ref.shape[0]
    offsets = code_ref.shape[0]
    small = pool_ref.shape[1] // LANES <= 8
    if small:
        for k in range(stack_ref.shape[0] // coeff):
            left = k * 2 * LANES
            part = pool_ref[:, left : min(left + 2 * LANES, pool_ref.shape[1])]
            if part.shape[1] < 2 * LANES:
                part = jnp.concatenate([part, jnp.zeros((coeff, LANES), jnp.bfloat16)], axis=1)
            stack_ref[k * coeff : (k + 1) * coeff, :] = part
    count_in_run = lax.broadcasted_iota(jnp.int32, (2 * LANES, LANES), 0).astype(jnp.int16)

    def picks(at, count):
        by_dot = min(BY_DOT, count) // 2 * 2 if small else 0
        done = 0
        for n in range(count - by_dot + by_dot // 2):
            total = count - by_dot + by_dot // 2
            pairs = by_dot // 2
            if (n + 1) * pairs // total > n * pairs // total:
                rows = [code_ref[pl.ds(at + done + m, 1), :] for m in (0, 1)]
                keep(at + done, pick_pair(rows, stack_ref, coeff, count_in_run))
                done += 2
            else:
                keep(at + done, [pick_lanes(code_ref[pl.ds(at + done, 1), :], pool_ref, coeff)])
                done += 1

    def keep(at, parts):
        for n, part in enumerate(parts):
            picked[pl.ds(pl.multiple_of((at + n) * coeff, coeff), coeff), :] = part

    def product(at, count):
        start = pl.multiple_of(at * coeff, LANES)
        return jnp.dot(
            matrix_ref[:, pl.ds(start, count * coeff)],
            picked[pl.ds(start, count * coeff), :],
            preferred_element_type=jnp.float32,
        )

    trips = offsets // GROUP
    rest = offsets - trips * GROUP
    picks(0, GROUP)

    def body(i, total):
        total += product((i - 1) * GROUP, GROUP)
        picks(i * GROUP, GROUP)
        return total

    total = lax.fori_loop(1, trips, body, jnp.zeros((coeff, LANES), jnp.float32))
    total += product((trips - 1) * GROUP, GROUP)
    if rest:
        picks(trips * GROUP, rest)
        total += product(trips * GROUP, rest)
    return total


def translate_scratch(offsets, coeff, lanes):
    return [
        pltpu.VMEM((offsets, LANES), jnp.int32),
        pltpu.VMEM((-(-lanes // (2 * LANES)) * coeff, 2 * LANES), jnp.bfloat16),
        pltpu.VMEM((offsets * coeff, LANES), jnp.bfloat16),
    ]


def own_kernel(
    me_ref, list_ref, matrix_ref, pool_ref, e_ref, d_hbm, out_ref, down_ref, code, stack, picked, d_ref, sem
):
    d_copy = pltpu.make_async_copy(d_hbm, d_ref, sem)
    d_copy.start()
    me = me_ref[0, 0]
    lists = list_ref[...]
    tiles = pool_ref.shape[1] // LANES
    other = (lists >> 7) ^ me
    tile = jnp.zeros_like(other)
    for bit in range(tiles.bit_length() - 1):
        tile = tile * 2 + ((other >> bit) & 1)
    code[...] = jnp.where(lists < tiles * LANES, tile * LANES + (lists & (LANES - 1)), -1)
    out_ref[...] = translate(OWN_GROUP, code, matrix_ref, pool_ref, stack, picked)
    d_copy.wait()
    down_ref[...] = lax.dot_general(
        d_ref[...], e_ref[...], (((1,), (1,)), ((), ())), preferred_element_type=jnp.float32
    ).astype(jnp.bfloat16)


def ghost_kernel(
    own_boxes, width, list_ref, matrix_ref, rows_ref, own_ref, down_ref, out_hbm,
    code, stack, picked, pool, extra, wide, out_ref, sems
):
    coeff = matrix_ref.shape[0]
    surface = out_ref.shape[0]
    lanes = rows_ref.shape[0]
    senders = lanes // ROWS
    more = width - ROWS
    lists = list_ref[...] - own_boxes
    sender = ((lists.astype(jnp.float32) + 0.5) * (1.0 / width)).astype(jnp.int32)
    slot = lists - sender * width
    place = jnp.where(
        slot < ROWS, sender * ROWS + slot, lanes + sender * more + slot - ROWS
    )
    code[...] = jnp.where((lists >= 0) & (lists < senders * width), place, -1)
    for at in range(0, lanes, LANES):
        turned = jnp.transpose(rows_ref[at : at + LANES, :].astype(jnp.float32)).astype(jnp.bfloat16)
        pool[:, at : at + LANES] = turned[0:coeff, :]
        extra[:, at : at + LANES] = turned[coeff : 2 * coeff, :]
    for at in range(0, pool.shape[1] - lanes, LANES):
        m = lax.broadcasted_iota(jnp.int32, (coeff, LANES), 1) + at
        source = (m >> (more.bit_length() - 1)) * ROWS + (m & (more - 1))
        lane, tile = (source & (LANES - 1)).astype(jnp.int16), (source >> 7).astype(jnp.int16)
        got = jnp.zeros((coeff, LANES), jnp.bfloat16)
        first = at // more * ROWS // LANES
        for k in range(first, min(first + LANES // more * ROWS // LANES, lanes // LANES)):
            part = lane_gather(extra[:, k * LANES : (k + 1) * LANES], lane)
            got = jnp.where(tile == jnp.int16(k), part, got)
        pool[:, lanes + at : lanes + at + LANES] = got
    total = translate(GHOST_GROUP, code, matrix_ref, pool, stack, picked)
    local_coeff = (total + own_ref[...]).astype(jnp.bfloat16)
    out_copies = []
    for at, size in chunks_of(surface, 96):
        wide[pl.ds(at * 8, size * 8), :] = jnp.dot(
            down_ref[pl.ds(at * 8, size * 8), :], local_coeff, preferred_element_type=jnp.float32
        )
        for c in range(8):
            out_ref[pl.ds(at, size), c * LANES : (c + 1) * LANES] = wide[
                pl.ds(at * 8 + c, size, stride=8), :
            ].astype(jnp.bfloat16)
        rows = pl.ds(at, size)
        out_copies.append(
            pltpu.make_async_copy(out_ref.at[rows, :], out_hbm.at[rows, :], sems.at[len(out_copies)])
        )
        out_copies[-1].start()
    for copy in out_copies:
        copy.wait()


def on_device(
    child_moments,
    upward_matrix,
    project_matrix,
    transfer_matrix,
    expand_matrix,
    downward_matrix,
    neighbour_list,
    ghost_map,
):
    surface = child_moments.shape[0]
    boxes = child_moments.shape[1] // 8
    coeff = project_matrix.shape[0]
    slots = ghost_map.shape[1]
    offsets = neighbour_list.shape[0]
    grp_count = lax.axis_size("grp")
    sub_count = lax.axis_size("sub")
    if boxes != LANES or sub_count & (sub_count - 1):
        raise ValueError("unsupported sizes")
    slot_lanes = -(-(slots + ROWS) // LANES) * LANES
    width = slots // grp_count
    more = width - ROWS
    if 2 * coeff != LANES or not 0 < more <= ROWS or more & (more - 1):
        raise ValueError("unsupported sizes")
    lane_tiles = -(-surface // LANES)
    packed, send = pl.pallas_call(
        functools.partial(upward_kernel, grp_count),
        out_shape=(
            jax.ShapeDtypeStruct((coeff, boxes), jnp.bfloat16),
            jax.ShapeDtypeStruct((sub_count * grp_count * ROWS, LANES), jnp.bfloat16),
        ),
        in_specs=[HBM] * 4,
        out_specs=(VMEM, VMEM),
        scratch_shapes=[
            pltpu.VMEM(child_moments.shape, jnp.bfloat16),
            pltpu.VMEM((surface * 8, surface), jnp.bfloat16),
            pltpu.VMEM(project_matrix.shape, jnp.bfloat16),
            pltpu.VMEM(ghost_map.shape, jnp.int32),
            pltpu.VMEM((1, slot_lanes), jnp.int32),
            pltpu.VMEM((lane_tiles, surface * 8, LANES), jnp.float32),
            pltpu.VMEM((surface, boxes), jnp.bfloat16),
            pltpu.VMEM((slot_lanes, coeff), jnp.float32),
            pltpu.SemaphoreType.DMA((3 + len(chunks_of(surface, 96)),)),
        ],
        compiler_params=pltpu.CompilerParams(vmem_limit_bytes=40000 << 10),
        cost_estimate=pl.CostEstimate(flops=500_000_000, bytes_accessed=3_000_000, transcendentals=0),
        name="upward",
    )(
        *(
            pltpu.with_memory_space_constraint(a, pltpu.HBM)
            for a in (
                child_moments,
                upward_matrix.reshape(surface * 8, surface),
                project_matrix,
                ghost_map,
            )
        )
    )
    received = lax.all_to_all(send, ("sub", "grp"), split_axis=0, concat_axis=0, tiled=True)
    own = packed
    hop = sub_count // 2
    while hop:
        other = lax.ppermute(own, "sub", [(i, i ^ hop) for i in range(sub_count)])
        own = jnp.concatenate([own, other], axis=1)
        hop //= 2
    me = lax.axis_index("sub").astype(jnp.int32).reshape(1, 1)
    own_part, down = pl.pallas_call(
        own_kernel,
        out_shape=(
            jax.ShapeDtypeStruct((coeff, boxes), jnp.float32),
            jax.ShapeDtypeStruct((surface * 8, coeff), jnp.bfloat16),
        ),
        in_specs=[SMEM, VMEM, VMEM, VMEM, VMEM, HBM],
        out_specs=(VMEM, VMEM),
        scratch_shapes=translate_scratch(offsets, coeff, own.shape[1])
        + [
            pltpu.VMEM((surface * 8, surface), jnp.bfloat16),
            pltpu.SemaphoreType.DMA(()),
        ],
        compiler_params=pltpu.CompilerParams(vmem_limit_bytes=24 << 20),
        cost_estimate=pl.CostEstimate(flops=3_000_000_000, bytes_accessed=1, transcendentals=0),
        name="own",
    )(
        me,
        neighbour_list,
        transfer_matrix,
        own,
        jnp.transpose(expand_matrix),
        pltpu.with_memory_space_constraint(downward_matrix.reshape(surface * 8, surface), pltpu.HBM),
    )
    sent_lanes = received.shape[0]
    ghost_lanes = sent_lanes + -(-(sent_lanes // ROWS * more) // LANES) * LANES
    result = pl.pallas_call(
        functools.partial(ghost_kernel, sub_count * boxes, width),
        out_shape=jax.ShapeDtypeStruct((surface, 8 * boxes), jnp.bfloat16),
        in_specs=[VMEM] * 5,
        out_specs=HBM,
        scratch_shapes=translate_scratch(offsets, coeff, ghost_lanes)
        + [
            pltpu.VMEM((coeff, ghost_lanes), jnp.bfloat16),
            pltpu.VMEM((coeff, sent_lanes), jnp.bfloat16),
            pltpu.VMEM((surface * 8, boxes), jnp.float32),
            pltpu.VMEM((surface, 8 * boxes), jnp.bfloat16),
            pltpu.SemaphoreType.DMA((len(chunks_of(surface, 96)),)),
        ],
        compiler_params=pltpu.CompilerParams(vmem_limit_bytes=24 << 20),
        name="ghost_downward",
    )(neighbour_list, transfer_matrix, received, own_part, down)
    return result


def solution(mesh):
    return jax.shard_map(
        on_device,
        mesh=mesh,
        in_specs=(
            P(None, ("grp", "sub")),
            P(),
            P(),
            P(),
            P(),
            P(),
            P(None, ("grp", "sub")),
            P(("grp", "sub"), None),
        ),
        out_specs=P(None, ("grp", "sub")),
        check_vma=False,
    )
```
